256 devices in a mesh: zero: 16 (over z, core), tp: 4 (over x), job: 4 (over y).
Axes of the slice: x: 4, y: 4, z: 8, core: 2. Of those that a mesh axis runs over, the one named last changes fastest.
Arguments:
- w_query: float32 [16384, 4096], P(('job', 'zero'), 'tp'), parts along dimension 0, may hold values from -0.125 to 0.125
- avg_query: float32 [16384, 4096], P(('job', 'zero'), 'tp'), parts along dimension 0, may hold values from -0.09375 to 0.09375
- w_key: float32 [16384, 1024], P(('job', 'zero'), 'tp'), parts along dimension 0, may hold values from -0.125 to 0.125
- avg_key: float32 [16384, 1024], P(('job', 'zero'), 'tp'), parts along dimension 0, may hold values from -0.09375 to 0.09375
- w_value: float32 [16384, 1024], P(('job', 'zero'), 'tp'), parts along dimension 0, may hold values from -0.125 to 0.125
- avg_value: float32 [16384, 1024], P(('job', 'zero'), 'tp'), parts along dimension 0, may hold values from -0.09375 to 0.09375
- norm_train: float32 [16384], P(('job', 'zero', 'tp')), parts along dimension 0, may hold values from 0.25 to 1.75
- norm_step: float32 [16384], P(('job', 'zero', 'tp')), parts along dimension 0, may hold values from -0.3 to 0.3
Outputs:
- serve_query: bfloat16 [16384, 4096], P('job', 'tp'), parts along dimension 0
- serve_key: bfloat16 [16384, 1024], P('job', 'tp'), parts along dimension 0
- serve_value: bfloat16 [16384, 1024], P('job', 'tp'), parts along dimension 0
- column_query: float32 [16384], P(('job', 'tp')), parts along dimension 0
- column_key: float32 [4096], P(('job', 'tp')), parts along dimension 0
- column_value: float32 [4096], P(('job', 'tp')), parts along dimension 0
- serve_norm: bfloat16 [16384], P('job'), parts along dimension 0
- fresh_query: float32 [16384, 4096], P(('job', 'zero'), 'tp'), parts along dimension 0
- fresh_key: float32 [16384, 1024], P(('job', 'zero'), 'tp'), parts along dimension 0
- fresh_value: float32 [16384, 1024], P(('job', 'zero'), 'tp'), parts along dimension 0
The draws below stay inside these ranges and needn't reach their ends.
There are 4 independent parts, one for each index of `job`. The reference program is written for one: setup_inputs(seed, part) draws one part's arguments, and reference() takes and returns one part's arrays. A program takes and returns all parts, laid end to end along the dimension named above; each array names one. Nothing has to cross between parts.
All inputs are finite; a program needn't handle non-finite values.
Results may differ from the reference program's by a relative error of at most 0.001.
Values may be sent and summed in bfloat16 or wider, within the bound.
No kernel may reach another device: no remote copies, remote signals or barrier semaphores. Data moves between devices by JAX's collectives and lax.ppermute only.
A program may use at most 128 MiB of HBM per device.

```python
import jax
import jax.numpy as jnp
from jax import lax

D_MODEL = 4096
Q_DIM = 4096
KV_DIM = 1024


def spiked(entries, rng, source, target, shards_of, factor):
    owner, partner = [(jnp.arange(entries.shape[axis_at]) // (entries.shape[axis_at] // shards_of)).reshape([-1 if axis == axis_at else 1 for axis in range(entries.ndim)]) for axis_at in (source, target)]
    chosen = jax.random.permutation(rng, shards_of)[partner]
    strong = (owner == chosen) | (owner == (partner + shards_of // 2) % shards_of)
    return jnp.where(strong, factor * entries, entries)


def levels(stream_key, extent, cuts, smallest, largest):
    factor_of, own = 1.0, jax.random.fold_in(stream_key, 6)
    for position, parts in cuts:
        heights = jnp.exp(jax.random.uniform(jax.random.fold_in(own, position), (parts,), jnp.float32, smallest / len(cuts), largest / len(cuts)))
        factor_of = factor_of * jnp.repeat(heights, extent[position] // parts).reshape([-1 if axis == position else 1 for axis in range(len(extent))])
    return factor_of


def bell_draw(key, shape, width, limit, pieces=(), kind=jnp.bfloat16):
    result = jax.random.normal(key, shape, jnp.float32) * width
    if len(pieces) > 0:
        result = levels(key, shape, pieces, -0.22, 0.18) * result
    return jnp.clip(result, min=-limit, max=limit).astype(kind)


def noise_with(key, extent, spread, bound, pieces, heavy, dtype=jnp.bfloat16):
    array = spread * jax.random.normal(key, extent, jnp.float32)
    if pieces:
        array = array * levels(key, extent, pieces, -0.22, 0.18)
    return jnp.clip(spiked(array, jax.random.fold_in(key, 3), *heavy), -bound, bound).astype(dtype)


def setup_inputs(seed: int = 0, part: int = 0) -> dict:
    splits = jax.random.split(jax.random.key(seed), 9)
    own_keys = jax.random.split(jax.random.fold_in(splits[8], part), 9)
    return {
        "w_query": noise_with(own_keys[0], (D_MODEL, Q_DIM), D_MODEL ** -0.5, 0.125, ((0, 16), (1, 4)), (0, 1, 16, 2.0), jnp.float32),
        "avg_query": bell_draw(own_keys[1], (D_MODEL, Q_DIM), D_MODEL ** -0.5, 0.09375, ((0, 16), (1, 4)), jnp.float32),
        "w_key": noise_with(own_keys[2], (D_MODEL, KV_DIM), D_MODEL ** -0.5, 0.125, ((0, 16), (1, 4)), (0, 1, 16, 2.0), jnp.float32),
        "avg_key": bell_draw(own_keys[3], (D_MODEL, KV_DIM), D_MODEL ** -0.5, 0.09375, ((0, 16), (1, 4)), jnp.float32),
        "w_value": noise_with(own_keys[4], (D_MODEL, KV_DIM), D_MODEL ** -0.5, 0.125, ((0, 16), (1, 4)), (0, 1, 16, 2.0), jnp.float32),
        "avg_value": bell_draw(own_keys[5], (D_MODEL, KV_DIM), D_MODEL ** -0.5, 0.09375, ((0, 16), (1, 4)), jnp.float32),
        "norm_train": jnp.clip(1.0 + 0.15 * jax.random.normal(own_keys[6], (D_MODEL,), jnp.float32), 0.25, 1.75),
        "norm_step": jnp.clip(jax.random.uniform(own_keys[7], (D_MODEL,), jnp.float32, -0.3, 0.3) * levels(own_keys[7], (D_MODEL,), ((0, 64),), -0.4, 0.0), -0.3, 0.3),
    }


keep_rate = 0.75

def reference(w_query, avg_query, w_key, avg_key, w_value, avg_value, norm_train, norm_step):
    fresh_query = keep_rate * avg_query + (1.0 - keep_rate) * w_query
    fresh_key = keep_rate * avg_key + (1.0 - keep_rate) * w_key
    fresh_value = keep_rate * avg_value + (1.0 - keep_rate) * w_value
    column_query = jnp.sqrt(lax.optimization_barrier(jnp.sum(fresh_query * fresh_query, axis=0)))
    serve_query = (fresh_query / column_query).astype(jnp.bfloat16)
    column_key = jnp.sqrt(lax.optimization_barrier(jnp.sum(fresh_key * fresh_key, axis=0)))
    serve_key = (fresh_key / column_key).astype(jnp.bfloat16)
    column_value = jnp.sqrt(lax.optimization_barrier(jnp.sum(fresh_value * fresh_value, axis=0)))
    serve_value = (fresh_value / column_value).astype(jnp.bfloat16)
    serve_norm = (norm_train + norm_step).astype(jnp.bfloat16)
    return (serve_query, serve_key, serve_value, column_query, column_key, column_value, serve_norm, fresh_query, fresh_key, fresh_value)
```

```python
import functools

import jax
import jax.numpy as jnp
from jax import lax
from jax.experimental import pallas as pl
from jax.experimental.pallas import tpu as pltpu
from jax.sharding import PartitionSpec as P

keep_rate = 0.75
CHIPS = 8
CORES = 2
PARTS = 2
GROUPS = ((0, 1, 2, 3), (4, 5), (6,), (7,))


def step_along(hops):
    return [
        (z * CORES + c, (z + hops) % CHIPS * CORES + c) for z in range(CHIPS) for c in range(CORES)
    ]


def other_core():
    return [(z * CORES + c, z * CORES + 1 - c) for z in range(CHIPS) for c in range(CORES)]


def normalise(everyone, query, key, value, *outs):
    pieces, (column_query, column_key, column_value, gain) = outs[: 2 * PARTS], outs[2 * PARTS :]
    wide, narrow = query.shape[1], key.shape[1]
    total = jnp.sum(everyone[...], axis=0, keepdims=True)
    column = jnp.sqrt(total[:, : wide + 2 * narrow])
    column_query[...] = column[:, :wide]
    column_key[...] = column[:, wide : wide + narrow]
    column_value[...] = column[:, wide + narrow :]
    mine = lax.axis_index("tp")
    own = everyone[:, wide + 2 * narrow :]
    size, each = own.shape
    twice = jnp.concatenate([own, own], axis=1).astype(jnp.bfloat16)
    tall = (2 * size, size)
    row, owner = (lax.broadcasted_iota(jnp.int32, tall, d) for d in (0, 1))
    spread = (row == 2 * owner + mine // 2).astype(jnp.bfloat16)
    moved = jnp.dot(spread, twice, preferred_element_type=jnp.float32)
    lane = lax.broadcasted_iota(jnp.int32, moved.shape, 1)
    gain[...] = jnp.where(lane // each == mine % 2, moved, 0.0).astype(gain.dtype)
    rows = pieces[0].shape[0]
    for i, piece in enumerate(pieces):
        at = slice(i * rows, (i + 1) * rows)
        piece[:, :wide] = (query[at] / column[:, :wide]).astype(piece.dtype)
        piece[:, wide : wide + narrow] = (key[at] / column[:, wide : wide + narrow]).astype(piece.dtype)
        piece[:, wide + narrow :] = (value[at] / column[:, wide + narrow :]).astype(piece.dtype)


def place(spots, *refs):
    n = len(spots)
    pieces, outs, sems = refs[:n], refs[-4:-1], refs[-1]
    me = lax.axis_index("zero")
    z, c = me // CORES, me % CORES
    copies = []
    for k, (hops, flip, at) in enumerate(spots):
        rows = pieces[k].shape[0]
        owner = (z + hops + CHIPS) % CHIPS * CORES + (1 - c if flip else c)
        row = pl.multiple_of(owner * (rows * 2 * PARTS) + at * rows, rows)
        column = 0
        for j, out in enumerate(outs):
            wide = out.shape[1]
            copies.append(
                pltpu.make_async_copy(
                    pieces[k].at[:, column : column + wide],
                    out.at[pl.ds(row, rows), :],
                    sems.at[k, j],
                )
            )
            column += wide
    for copy in copies:
        copy.start()
    for copy in copies:
        copy.wait()


def placed(pieces, spots, outs, shapes):
    n = len(pieces)
    before = () if outs is None else tuple(outs)
    size = sum(p.size * 2 for p in pieces)
    pieces = [pltpu.with_memory_space_constraint(p, pltpu.VMEM) for p in pieces]
    return pl.pallas_call(
        functools.partial(place, spots),
        out_shape=shapes,
        in_specs=[pl.BlockSpec(memory_space=pltpu.VMEM)] * n
        + [pl.BlockSpec(memory_space=pl.ANY)] * len(before),
        out_specs=[pl.BlockSpec(memory_space=pl.ANY)] * 3,
        scratch_shapes=[pltpu.SemaphoreType.DMA((n, 3))],
        input_output_aliases={n + j: j for j in range(len(before))},
        cost_estimate=pl.CostEstimate(flops=0, bytes_accessed=2 * size, transcendentals=0),
        compiler_params=pltpu.CompilerParams(vmem_limit_bytes=12 << 20),
        name="place",
    )(*pieces, *before)


def body(w_query, avg_query, w_key, avg_key, w_value, avg_value, norm_train, norm_step):
    fresh_query = keep_rate * avg_query + (1.0 - keep_rate) * w_query
    fresh_key = keep_rate * avg_key + (1.0 - keep_rate) * w_key
    fresh_value = keep_rate * avg_value + (1.0 - keep_rate) * w_value
    depth, wide = fresh_query.shape
    narrow = fresh_key.shape[1]
    gain = (norm_train + norm_step).astype(jnp.bfloat16)
    line = jnp.concatenate(
        [
            jnp.sum(fresh_query * fresh_query, axis=0),
            jnp.sum(fresh_key * fresh_key, axis=0),
            jnp.sum(fresh_value * fresh_value, axis=0),
            gain.astype(jnp.float32),
        ]
    )
    copies = jnp.broadcast_to(line, (CHIPS * CORES, line.size))
    everyone = lax.all_to_all(copies, "zero", split_axis=0, concat_axis=0, tiled=True)

    rows, full = depth // (2 * PARTS), wide + 2 * narrow
    vm = pl.BlockSpec(memory_space=pltpu.VMEM)
    *pieces, column_query, column_key, column_value, gains = pl.pallas_call(
        normalise,
        out_shape=[pltpu.VMEM((rows, full), jnp.bfloat16)] * (2 * PARTS)
        + [jax.ShapeDtypeStruct((1, n), jnp.float32) for n in (wide, narrow, narrow)]
        + [pltpu.VMEM((2 * CHIPS * CORES, 2 * gain.size), jnp.bfloat16)],
        in_specs=[vm] * 4,
        out_specs=[vm] * (2 * PARTS + 4),
        compiler_params=pltpu.CompilerParams(vmem_limit_bytes=8 << 20),
        name="normalise",
    )(
        everyone,
        *(pltpu.with_memory_space_constraint(a, pltpu.VMEM) for a in (fresh_query, fresh_key, fresh_value)),
    )

    size = CHIPS * CORES
    forth, back = list(pieces[:PARTS]), list(pieces[PARTS:])
    held = {}
    held[0] = []
    for i in range(PARTS):
        for which, at in ((forth[i], i), (back[i], PARTS + i)):
            held[0].append((which, (0, False, at)))
            held[0].append((lax.ppermute(which, "zero", other_core()), (0, True, at)))
    for hop in range(1, CHIPS):
        held[hop] = []
        for i in range(PARTS):
            forth[i] = lax.ppermute(forth[i], "zero", step_along(1))
            back[i] = lax.ppermute(back[i], "zero", step_along(-1))
            for which, to, at in ((forth[i], -hop, i), (back[i], hop, PARTS + i)):
                held[hop].append((which, (to, False, at)))
                held[hop].append((lax.ppermute(which, "zero", other_core()), (to, True, at)))

    shapes = [jax.ShapeDtypeStruct((depth * size, n), jnp.bfloat16) for n in (wide, narrow, narrow)]
    outs = None
    for group in GROUPS:
        some = [p for hop in group for p in held[hop]]
        outs = placed([p for p, _ in some], [s for _, s in some], outs, shapes)
    serve_query, serve_key, serve_value = outs

    tp = lax.axis_size("tp")
    serve_norm = gains
    for k in range(1, tp):
        serve_norm += lax.ppermute(gains, "tp", [(i, (i + k) % tp) for i in range(tp)])
    serve_norm = serve_norm.reshape(-1)
    return (
        serve_query,
        serve_key,
        serve_value,
        column_query.reshape(-1),
        column_key.reshape(-1),
        column_value.reshape(-1),
        serve_norm,
        fresh_query,
        fresh_key,
        fresh_value,
    )


def solution(mesh):
    in_specs = (
        P(("job", "zero"), "tp"),
        P(("job", "zero"), "tp"),
        P(("job", "zero"), "tp"),
        P(("job", "zero"), "tp"),
        P(("job", "zero"), "tp"),
        P(("job", "zero"), "tp"),
        P(("job", "zero", "tp")),
        P(("job", "zero", "tp")),
    )
    out_specs = (
        P("job", "tp"),
        P("job", "tp"),
        P("job", "tp"),
        P(("job", "tp")),
        P(("job", "tp")),
        P(("job", "tp")),
        P("job"),
        P(("job", "zero"), "tp"),
        P(("job", "zero"), "tp"),
        P(("job", "zero"), "tp"),
    )
    return jax.shard_map(body, mesh=mesh, in_specs=in_specs, out_specs=out_specs, check_vma=False)
```

```python
import functools

import jax
import jax.numpy as jnp
from jax import lax
from jax.experimental import pallas as pl
from jax.experimental.pallas import tpu as pltpu
from jax.sharding import PartitionSpec as P


keep_rate = 0.75
CHIPS = 8
CORES = 2


def both_ways():
    return [
        (z * CORES + c, (z + 1 - 2 * c) % CHIPS * CORES + c) for z in range(CHIPS) for c in range(CORES)
    ]


def other_core():
    return [(z * CORES + c, z * CORES + 1 - c) for z in range(CHIPS) for c in range(CORES)]


def normalise(everyone, query, key, value, *outs):
    pieces, (column_query, column_key, column_value, gain) = outs[:2], outs[2:]
    wide, narrow = query.shape[1], key.shape[1]
    total = jnp.sum(everyone[...], axis=0, keepdims=True)
    column = jnp.sqrt(total[:, : wide + 2 * narrow])
    column_query[...] = column[:, :wide]
    column_key[...] = column[:, wide : wide + narrow]
    column_value[...] = column[:, wide + narrow :]
    mine = lax.axis_index("tp")
    own = everyone[:, wide + 2 * narrow :]
    size, each = own.shape
    twice = jnp.concatenate([own, own], axis=1).astype(jnp.bfloat16)
    tall = (2 * size, size)
    row, owner = (lax.broadcasted_iota(jnp.int32, tall, d) for d in (0, 1))
    spread = (row == 2 * owner + mine // 2).astype(jnp.bfloat16)
    moved = jnp.dot(spread, twice, preferred_element_type=jnp.float32)
    lane = lax.broadcasted_iota(jnp.int32, moved.shape, 1)
    gain[...] = jnp.where(lane // each == mine % 2, moved, 0.0).astype(gain.dtype)
    rows = pieces[0].shape[0]
    core = lax.axis_index("zero") % CORES
    for piece, half in zip(pieces, (core, 1 - core)):
        at = pl.ds(pl.multiple_of(half * rows, rows), rows)
        piece[:, :wide] = (query[at] / column[:, :wide]).astype(piece.dtype)
        piece[:, wide : wide + narrow] = (key[at] / column[:, wide : wide + narrow]).astype(piece.dtype)
        piece[:, wide + narrow :] = (value[at] / column[:, wide + narrow :]).astype(piece.dtype)


def place(spots, *refs):
    n = len(spots)
    pieces, outs, sems = refs[:n], refs[-4:-1], refs[-1]
    me = lax.axis_index("zero")
    z, c = me // CORES, me % CORES
    copies = []
    for k, (hops, theirs, other) in enumerate(spots):
        rows = pieces[k].shape[0]
        half = 1 - c if theirs else c
        shard = 1 - c if other else c
        chip = (z - hops * (1 - 2 * half) + CHIPS) % CHIPS
        row = pl.multiple_of(((chip * CORES + shard) * 2 + half) * rows, rows)
        column = 0
        for j, out in enumerate(outs):
            wide = out.shape[1]
            copies.append(
                pltpu.make_async_copy(
                    pieces[k].at[:, column : column + wide],
                    out.at[pl.ds(row, rows), :],
                    sems.at[k, j],
                )
            )
            column += wide
    for copy in copies:
        copy.start()
    for copy in copies:
        copy.wait()


def placed(pieces, spots, outs, shapes):
    n = len(pieces)
    before = () if outs is None else tuple(outs)
    size = sum(p.size * 2 for p in pieces)
    pieces = [pltpu.with_memory_space_constraint(p, pltpu.VMEM) for p in pieces]
    return pl.pallas_call(
        functools.partial(place, spots),
        out_shape=shapes,
        in_specs=[pl.BlockSpec(memory_space=pltpu.VMEM)] * n
        + [pl.BlockSpec(memory_space=pl.ANY)] * len(before),
        out_specs=[pl.BlockSpec(memory_space=pl.ANY)] * 3,
        scratch_shapes=[pltpu.SemaphoreType.DMA((n, 3))],
        input_output_aliases={n + j: j for j in range(len(before))},
        cost_estimate=pl.CostEstimate(flops=0, bytes_accessed=2 * size, transcendentals=0),
        compiler_params=pltpu.CompilerParams(vmem_limit_bytes=12 << 20),
        name="place",
    )(*pieces, *before)


def body(w_query, avg_query, w_key, avg_key, w_value, avg_value, norm_train, norm_step):
    fresh_query = keep_rate * avg_query + (1.0 - keep_rate) * w_query
    fresh_key = keep_rate * avg_key + (1.0 - keep_rate) * w_key
    fresh_value = keep_rate * avg_value + (1.0 - keep_rate) * w_value
    depth, wide = fresh_query.shape
    narrow = fresh_key.shape[1]
    gain = (norm_train + norm_step).astype(jnp.bfloat16)
    line = jnp.concatenate(
        [
            jnp.sum(fresh_query * fresh_query, axis=0),
            jnp.sum(fresh_key * fresh_key, axis=0),
            jnp.sum(fresh_value * fresh_value, axis=0),
            gain.astype(jnp.float32),
        ]
    )
    copies = jnp.broadcast_to(line, (CHIPS * CORES, line.size))
    everyone = lax.all_to_all(copies, "zero", split_axis=0, concat_axis=0, tiled=True)

    rows, full = depth // 2, wide + 2 * narrow
    vm = pl.BlockSpec(memory_space=pltpu.VMEM)
    keep, give, column_query, column_key, column_value, gains = pl.pallas_call(
        normalise,
        out_shape=[pltpu.VMEM((rows, full), jnp.bfloat16)] * 2
        + [jax.ShapeDtypeStruct((1, n), jnp.float32) for n in (wide, narrow, narrow)]
        + [pltpu.VMEM((2 * CHIPS * CORES, 2 * gain.size), jnp.bfloat16)],
        in_specs=[vm] * 4,
        out_specs=[vm] * 6,
        compiler_params=pltpu.CompilerParams(vmem_limit_bytes=8 << 20),
        name="normalise",
    )(
        everyone,
        *(pltpu.with_memory_space_constraint(a, pltpu.VMEM) for a in (fresh_query, fresh_key, fresh_value)),
    )

    size = CHIPS * CORES
    def swap(piece):
        return lax.ppermute(piece, "zero", other_core())

    near, far = keep, swap(give)
    held = [
        [
            (keep, (0, False, False)),
            (far, (0, False, True)),
            (swap(keep), (0, True, True)),
            (give, (0, True, False)),
        ]
    ]
    for hop in range(1, CHIPS):
        near = lax.ppermute(near, "zero", both_ways())
        far = lax.ppermute(far, "zero", both_ways())
        held.append(
            [
                (near, (hop, False, False)),
                (far, (hop, False, True)),
                (swap(near), (hop, True, True)),
                (swap(far), (hop, True, False)),
            ]
        )

    shapes = [jax.ShapeDtypeStruct((depth * size, n), jnp.bfloat16) for n in (wide, narrow, narrow)]
    outs = None
    for some in held:
        for two in (some[::2], some[1::2]):
            outs = placed([p for p, _ in two], [s for _, s in two], outs, shapes)
    serve_query, serve_key, serve_value = outs

    tp = lax.axis_size("tp")
    serve_norm = gains
    for k in range(1, tp):
        theirs = lax.ppermute(gains, "tp", [(i, (i + k) % tp) for i in range(tp)])
        serve_norm += theirs
    serve_norm = serve_norm.reshape(-1)
    return (
        serve_query,
        serve_key,
        serve_value,
        column_query.reshape(-1),
        column_key.reshape(-1),
        column_value.reshape(-1),
        serve_norm,
        fresh_query,
        fresh_key,
        fresh_value,
    )


def solution(mesh):
    in_specs = (
        P(("job", "zero"), "tp"),
        P(("job", "zero"), "tp"),
        P(("job", "zero"), "tp"),
        P(("job", "zero"), "tp"),
        P(("job", "zero"), "tp"),
        P(("job", "zero"), "tp"),
        P(("job", "zero", "tp")),
        P(("job", "zero", "tp")),
    )
    out_specs = (
        P("job", "tp"),
        P("job", "tp"),
        P("job", "tp"),
        P(("job", "tp")),
        P(("job", "tp")),
        P(("job", "tp")),
        P("job"),
        P(("job", "zero"), "tp"),
        P(("job", "zero"), "tp"),
        P(("job", "zero"), "tp"),
    )
    return jax.shard_map(body, mesh=mesh, in_specs=in_specs, out_specs=out_specs, check_vma=False)
```

```python
import functools

import jax
import jax.numpy as jnp
from jax import lax
from jax.experimental import pallas as pl
from jax.experimental.pallas import tpu as pltpu
from jax.sharding import PartitionSpec as P


keep_rate = 0.75
CHIPS = 8
CORES = 2
LAST = CHIPS - 1


def both_ways():
    return [
        (z * CORES + c, (z + 1 - 2 * c) % CHIPS * CORES + c) for z in range(CHIPS) for c in range(CORES)
    ]


def other_core():
    return [(z * CORES + c, z * CORES + 1 - c) for z in range(CHIPS) for c in range(CORES)]


def pack(query, key, value, out):
    wide, narrow, half = query.shape[1], key.shape[1], query.shape[0] // CORES
    at = pl.ds(pl.multiple_of(lax.axis_index("zero") % CORES * half, half), out.shape[0])
    out[:, :wide] = query[at]
    out[:, wide : wide + narrow] = key[at]
    out[:, wide + narrow :] = value[at]


def join(*refs):
    *parts, line = refs
    at = 0
    for part in parts:
        line[:, at : at + part.shape[1]] = part[...]
        at += part.shape[1]


def stack(first, second, out):
    rows = first.shape[0]
    out[:rows] = first[...]
    out[rows:] = second[...]


def stacked(first, second):
    vm = pl.BlockSpec(memory_space=pltpu.VMEM)
    return pl.pallas_call(
        stack,
        out_shape=pltpu.VMEM((2 * first.shape[0], first.shape[1]), first.dtype),
        in_specs=[vm] * 2,
        out_specs=vm,
        compiler_params=pltpu.CompilerParams(vmem_limit_bytes=1 << 20),
        name="stack",
    )(*(pltpu.with_memory_space_constraint(a, pltpu.VMEM) for a in (first, second)))


def tick(*refs):
    del refs


def ticked(outs):
    where = [pl.BlockSpec(memory_space=pl.ANY)] * len(outs)
    return pl.pallas_call(
        tick,
        out_shape=[jax.ShapeDtypeStruct(a.shape, a.dtype) for a in outs],
        in_specs=where,
        out_specs=where,
        input_output_aliases={j: j for j in range(len(outs))},
        compiler_params=pltpu.CompilerParams(vmem_limit_bytes=1 << 20),
        name="tick",
    )(*outs)


def receive(early, column_query, column_key, column_value, out):
    at = 0
    for column in (column_query, column_key, column_value):
        here = slice(at, at + column.shape[1])
        out[:, here] = (early[:, here] / column[...]).astype(out.dtype)
        at += column.shape[1]


def normalise(everyone, query, key, value, *outs):
    pieces, (late, *gives), columns, gain = outs[:2], outs[2:5], outs[5:11], outs[11]
    wide, narrow = query.shape[1], key.shape[1]
    total = jnp.sum(everyone[...], axis=0, keepdims=True)
    column = jnp.sqrt(total[:, : wide + 2 * narrow])
    for here in (columns[:3], columns[3:]):
        here[0][...] = column[:, :wide]
        here[1][...] = column[:, wide : wide + narrow]
        here[2][...] = column[:, wide + narrow :]
    tp = lax.axis_index("tp")
    own = everyone[:, wide + 2 * narrow :]
    size, each = own.shape
    twice = jnp.concatenate([own, own], axis=1).astype(jnp.bfloat16)
    tall = (2 * size, size)
    row, owner = (lax.broadcasted_iota(jnp.int32, tall, d) for d in (0, 1))
    spread = (row == 2 * owner + tp // 2).astype(jnp.bfloat16)
    moved = jnp.dot(spread, twice, preferred_element_type=jnp.float32)
    lane = lax.broadcasted_iota(jnp.int32, moved.shape, 1)
    gain[...] = jnp.where(lane // each == tp % 2, moved, 0.0).astype(gain.dtype)
    rows = pieces[0].shape[0]
    core = lax.axis_index("zero") % CORES
    for piece, half in zip(pieces, (core, 1 - core)):
        at = pl.ds(pl.multiple_of(half * rows, rows), rows)
        piece[:, :wide] = (query[at] / column[:, :wide]).astype(piece.dtype)
        piece[:, wide : wide + narrow] = (key[at] / column[:, wide : wide + narrow]).astype(piece.dtype)
        piece[:, wide + narrow :] = (value[at] / column[:, wide + narrow :]).astype(piece.dtype)
    half = late.shape[0]
    late[...] = pieces[0][half:]
    gives[0][...] = pieces[1][:half]
    gives[1][...] = pieces[1][half:]


def place(spots, *refs):
    n = len(spots)
    pieces, outs, sems = refs[:n], refs[-4:-1], refs[-1]
    me = lax.axis_index("zero")
    z, c = me // CORES, me % CORES
    copies = []
    for k, (hops, theirs, other, part) in enumerate(spots):
        rows = pieces[k].shape[0]
        half = 1 - c if theirs else c
        shard = 1 - c if other else c
        chip = (z - hops * (1 - 2 * half) + CHIPS) % CHIPS
        unit = outs[0].shape[0] // (CHIPS * CORES * 2)
        row = pl.multiple_of(((chip * CORES + shard) * 2 + half) * unit + part * rows, rows)
        column = 0
        for j, out in enumerate(outs):
            wide = out.shape[1]
            copies.append(
                pltpu.make_async_copy(
                    pieces[k].at[:, column : column + wide],
                    out.at[pl.ds(row, rows), :],
                    sems.at[k, j],
                )
            )
            column += wide
    for copy in copies:
        copy.start()
    for copy in copies:
        copy.wait()


def placed(pieces, spots, outs, shapes):
    n = len(pieces)
    before = () if outs is None else tuple(outs)
    size = sum(p.size * 2 for p in pieces)
    pieces = [pltpu.with_memory_space_constraint(p, pltpu.VMEM) for p in pieces]
    return pl.pallas_call(
        functools.partial(place, spots),
        out_shape=shapes,
        in_specs=[pl.BlockSpec(memory_space=pltpu.VMEM)] * n
        + [pl.BlockSpec(memory_space=pl.ANY)] * len(before),
        out_specs=[pl.BlockSpec(memory_space=pl.ANY)] * 3,
        scratch_shapes=[pltpu.SemaphoreType.DMA((n, 3))],
        input_output_aliases={n + j: j for j in range(len(before))},
        cost_estimate=pl.CostEstimate(flops=0, bytes_accessed=2 * size, transcendentals=0),
        compiler_params=pltpu.CompilerParams(vmem_limit_bytes=12 << 20),
        name="place",
    )(*pieces, *before)


def body(w_query, avg_query, w_key, avg_key, w_value, avg_value, norm_train, norm_step):
    fresh_query = keep_rate * avg_query + (1.0 - keep_rate) * w_query
    fresh_key = keep_rate * avg_key + (1.0 - keep_rate) * w_key
    fresh_value = keep_rate * avg_value + (1.0 - keep_rate) * w_value
    depth, wide = fresh_query.shape
    narrow = fresh_key.shape[1]
    gain = (norm_train + norm_step).astype(jnp.bfloat16)
    rows, full = depth // 2, wide + 2 * narrow
    vm = pl.BlockSpec(memory_space=pltpu.VMEM)
    fresh = [pltpu.with_memory_space_constraint(a, pltpu.VMEM) for a in (fresh_query, fresh_key, fresh_value)]
    early = pl.pallas_call(
        pack,
        out_shape=pltpu.VMEM((rows // 2, full), jnp.float32),
        in_specs=[vm] * 3,
        out_specs=vm,
        compiler_params=pltpu.CompilerParams(vmem_limit_bytes=8 << 20),
        name="pack",
    )(*fresh)
    early = lax.ppermute(early, "zero", both_ways())
    parts = [
        *(jnp.sum(a * a, axis=0, keepdims=True) for a in (fresh_query, fresh_key, fresh_value)),
        gain.astype(jnp.float32).reshape(1, -1),
    ]
    line = pl.pallas_call(
        join,
        out_shape=pltpu.VMEM((1, full + gain.size), jnp.float32),
        in_specs=[vm] * 4,
        out_specs=vm,
        compiler_params=pltpu.CompilerParams(vmem_limit_bytes=1 << 20),
        name="join",
    )(*(pltpu.with_memory_space_constraint(a, pltpu.VMEM) for a in parts))
    copies = jnp.broadcast_to(line, (CHIPS * CORES, line.size))
    everyone = lax.all_to_all(copies, "zero", split_axis=0, concat_axis=0, tiled=True)
    keep, give, late, *gives, q, k, v, q_out, k_out, v_out, gains = pl.pallas_call(
        normalise,
        out_shape=[pltpu.VMEM((rows, full), jnp.bfloat16)] * 2
        + [pltpu.VMEM((rows // 2, full), jnp.bfloat16)] * 3
        + [pltpu.VMEM((1, n), jnp.float32) for n in (wide, narrow, narrow)]
        + [jax.ShapeDtypeStruct((1, n), jnp.float32) for n in (wide, narrow, narrow)]
        + [pltpu.VMEM((2 * CHIPS * CORES, 2 * gain.size), jnp.bfloat16)],
        in_specs=[vm] * 4,
        out_specs=[vm] * 12,
        compiler_params=pltpu.CompilerParams(vmem_limit_bytes=8 << 20),
        name="normalise",
    )(everyone, *fresh)
    near = pl.pallas_call(
        receive,
        out_shape=pltpu.VMEM((rows // 2, full), jnp.bfloat16),
        in_specs=[vm] * 4,
        out_specs=vm,
        compiler_params=pltpu.CompilerParams(vmem_limit_bytes=8 << 20),
        name="receive",
    )(*(pltpu.with_memory_space_constraint(a, pltpu.VMEM) for a in (early, q, k, v)))

    size = CHIPS * CORES

    def swap(piece):
        return lax.ppermute(piece, "zero", other_core())

    have = {("a", 1): near, ("b", 0): late}
    have["c", 0], have["d", 0] = (swap(g) for g in gives)
    for kind in "abcd":
        for hop in range(1 + (kind == "a"), CHIPS):
            have[kind, hop] = lax.ppermute(have[kind, hop - 1], "zero", both_ways())
    hands = {"hand0": swap(keep)}
    for hop in range(1, CHIPS):
        for kind, pair in (("near", "ab"), ("far", "cd")):
            if hop == LAST and kind == "far":
                continue
            both = stacked(*(have[p, hop] for p in pair))
            hands[f"{kind}{hop}"] = swap(both)
    for kind in "cd":
        hands[f"{kind}{LAST}"] = swap(have[kind, LAST])

    def mine(kind, hop):
        return have[kind, hop], (hop, False, kind in "cd", "abcd".index(kind) % 2)

    def theirs(kind, hop):
        return hands[f"{kind}{hop}"], (hop, True, kind == "near", 0)

    puts = [
        [
            (keep, (0, False, False, 0)),
            (give, (0, True, False, 0)),
            (have["c", 0], (0, False, True, 0)),
            (have["d", 0], (0, False, True, 1)),
        ],
        [],
        [mine("a", 1), mine("a", 2), mine("b", 1), (hands["hand0"], (0, True, True, 0))],
        [],
        [mine("c", 1), mine("d", 1)],
    ]
    for hop in range(2, LAST):
        puts += [
            [],
            [mine("a", hop + 1), mine("b", hop), theirs("near", hop - 1), theirs("far", hop - 1)],
            [],
            [mine("c", hop), mine("d", hop)],
        ]
    puts += [
        [theirs("near", LAST - 1), theirs("far", LAST - 1)],
        [mine("b", LAST)],
        [theirs("near", LAST), mine("c", LAST)],
        [(hands[f"c{LAST}"], (LAST, True, False, 0)), mine("d", LAST)],
        [(hands[f"d{LAST}"], (LAST, True, False, 1))],
    ]

    shapes = [jax.ShapeDtypeStruct((depth * size, n), jnp.bfloat16) for n in (wide, narrow, narrow)]
    outs = None
    for some in puts:
        outs = placed([p for p, _ in some], [s for _, s in some], outs, shapes) if some else ticked(outs)
    serve_query, serve_key, serve_value = outs

    tp = lax.axis_size("tp")
    serve_norm = gains
    for k in (1, 2):
        theirs = lax.ppermute(serve_norm, "tp", [(i, i ^ k) for i in range(tp)])
        serve_norm += theirs
    serve_norm = serve_norm.reshape(-1)
    return (
        serve_query,
        serve_key,
        serve_value,
        *(column.reshape(-1) for column in (q_out, k_out, v_out)),
        serve_norm,
        fresh_query,
        fresh_key,
        fresh_value,
    )


def solution(mesh):
    in_specs = (
        P(("job", "zero"), "tp"),
        P(("job", "zero"), "tp"),
        P(("job", "zero"), "tp"),
        P(("job", "zero"), "tp"),
        P(("job", "zero"), "tp"),
        P(("job", "zero"), "tp"),
        P(("job", "zero", "tp")),
        P(("job", "zero", "tp")),
    )
    out_specs = (
        P("job", "tp"),
        P("job", "tp"),
        P("job", "tp"),
        P(("job", "tp")),
        P(("job", "tp")),
        P(("job", "tp")),
        P("job"),
        P(("job", "zero"), "tp"),
        P(("job", "zero"), "tp"),
        P(("job", "zero"), "tp"),
    )
    return jax.shard_map(body, mesh=mesh, in_specs=in_specs, out_specs=out_specs, check_vma=False)
```

```python
import functools

import jax
import jax.numpy as jnp
from jax import lax
from jax.experimental import pallas as pl
from jax.experimental.pallas import tpu as pltpu
from jax.sharding import PartitionSpec as P


keep_rate = 0.75
CHIPS = 8
CORES = 2
LAST = CHIPS - 1


def both_ways():
    return [
        (z * CORES + c, (z + 1 - 2 * c) % CHIPS * CORES + c) for z in range(CHIPS) for c in range(CORES)
    ]


def other_core():
    return [(z * CORES + c, z * CORES + 1 - c) for z in range(CHIPS) for c in range(CORES)]


def pack(query, key, value, out):
    wide, narrow, half = query.shape[1], key.shape[1], query.shape[0] // CORES
    at = pl.ds(pl.multiple_of(lax.axis_index("zero") % CORES * half, half), out.shape[0])
    out[:, :wide] = query[at]
    out[:, wide : wide + narrow] = key[at]
    out[:, wide + narrow :] = value[at]


def join(*refs):
    *parts, line = refs
    at = 0
    for part in parts:
        line[:, at : at + part.shape[1]] = part[...]
        at += part.shape[1]


def stack(first, second, out):
    rows = first.shape[0]
    out[:rows] = first[...]
    out[rows:] = second[...]


def stacked(first, second):
    vm = pl.BlockSpec(memory_space=pltpu.VMEM)
    return pl.pallas_call(
        stack,
        out_shape=pltpu.VMEM((2 * first.shape[0], first.shape[1]), first.dtype),
        in_specs=[vm] * 2,
        out_specs=vm,
        compiler_params=pltpu.CompilerParams(vmem_limit_bytes=1 << 20),
        name="stack",
    )(*(pltpu.with_memory_space_constraint(a, pltpu.VMEM) for a in (first, second)))


def tick(*refs):
    del refs


def ticked(outs):
    where = [pl.BlockSpec(memory_space=pl.ANY)] * len(outs)
    return pl.pallas_call(
        tick,
        out_shape=[jax.ShapeDtypeStruct(a.shape, a.dtype) for a in outs],
        in_specs=where,
        out_specs=where,
        input_output_aliases={j: j for j in range(len(outs))},
        compiler_params=pltpu.CompilerParams(vmem_limit_bytes=1 << 20),
        name="tick",
    )(*outs)


def receive(early, column_query, column_key, column_value, out):
    at = 0
    for column in (column_query, column_key, column_value):
        here = slice(at, at + column.shape[1])
        out[:, here] = (early[:, here] / column[...]).astype(out.dtype)
        at += column.shape[1]


def normalise(everyone, query, key, value, *outs):
    pieces, (late, *gives), columns, gain = outs[:2], outs[2:5], outs[5:11], outs[11]
    wide, narrow = query.shape[1], key.shape[1]
    total = jnp.sum(everyone[...], axis=0, keepdims=True)
    column = jnp.sqrt(total[:, : wide + 2 * narrow])
    for here in (columns[:3], columns[3:]):
        here[0][...] = column[:, :wide]
        here[1][...] = column[:, wide : wide + narrow]
        here[2][...] = column[:, wide + narrow :]
    tp = lax.axis_index("tp")
    own = everyone[:, wide + 2 * narrow :]
    size, each = own.shape
    twice = jnp.concatenate([own, own], axis=1).astype(jnp.bfloat16)
    tall = (2 * size, size)
    row, owner = (lax.broadcasted_iota(jnp.int32, tall, d) for d in (0, 1))
    spread = (row == 2 * owner + tp // 2).astype(jnp.bfloat16)
    moved = jnp.dot(spread, twice, preferred_element_type=jnp.float32)
    lane = lax.broadcasted_iota(jnp.int32, moved.shape, 1)
    gain[...] = jnp.where(lane // each == tp % 2, moved, 0.0).astype(gain.dtype)
    rows = pieces[0].shape[0]
    core = lax.axis_index("zero") % CORES
    for piece, half in zip(pieces, (core, 1 - core)):
        at = pl.ds(pl.multiple_of(half * rows, rows), rows)
        piece[:, :wide] = (query[at] / column[:, :wide]).astype(piece.dtype)
        piece[:, wide : wide + narrow] = (key[at] / column[:, wide : wide + narrow]).astype(piece.dtype)
        piece[:, wide + narrow :] = (value[at] / column[:, wide + narrow :]).astype(piece.dtype)
    half = late.shape[0]
    late[...] = pieces[0][half:]
    gives[0][...] = pieces[1][:half]
    gives[1][...] = pieces[1][half:]


def place(spots, *refs):
    n = len(spots)
    pieces, outs, sems = refs[:n], refs[-4:-1], refs[-1]
    me = lax.axis_index("zero")
    z, c = me // CORES, me % CORES
    copies = []
    for k, (hops, theirs, other, part) in enumerate(spots):
        rows = pieces[k].shape[0]
        half = 1 - c if theirs else c
        shard = 1 - c if other else c
        chip = (z - hops * (1 - 2 * half) + CHIPS) % CHIPS
        unit = outs[0].shape[0] // (CHIPS * CORES * 2)
        row = pl.multiple_of(((chip * CORES + shard) * 2 + half) * unit + part * rows, rows)
        column = 0
        for j, out in enumerate(outs):
            wide = out.shape[1]
            copies.append(
                pltpu.make_async_copy(
                    pieces[k].at[:, column : column + wide],
                    out.at[pl.ds(row, rows), :],
                    sems.at[k, j],
                )
            )
            column += wide
    for copy in copies:
        copy.start()
    for copy in copies:
        copy.wait()


def placed(pieces, spots, outs, shapes):
    n = len(pieces)
    before = () if outs is None else tuple(outs)
    size = sum(p.size * 2 for p in pieces)
    pieces = [pltpu.with_memory_space_constraint(p, pltpu.VMEM) for p in pieces]
    return pl.pallas_call(
        functools.partial(place, spots),
        out_shape=shapes,
        in_specs=[pl.BlockSpec(memory_space=pltpu.VMEM)] * n
        + [pl.BlockSpec(memory_space=pl.ANY)] * len(before),
        out_specs=[pl.BlockSpec(memory_space=pl.ANY)] * 3,
        scratch_shapes=[pltpu.SemaphoreType.DMA((n, 3))],
        input_output_aliases={n + j: j for j in range(len(before))},
        cost_estimate=pl.CostEstimate(flops=0, bytes_accessed=2 * size, transcendentals=0),
        compiler_params=pltpu.CompilerParams(vmem_limit_bytes=12 << 20),
        name="place",
    )(*pieces, *before)


def body(w_query, avg_query, w_key, avg_key, w_value, avg_value, norm_train, norm_step):
    fresh_query = keep_rate * avg_query + (1.0 - keep_rate) * w_query
    fresh_key = keep_rate * avg_key + (1.0 - keep_rate) * w_key
    fresh_value = keep_rate * avg_value + (1.0 - keep_rate) * w_value
    depth, wide = fresh_query.shape
    narrow = fresh_key.shape[1]
    gain = (norm_train + norm_step).astype(jnp.bfloat16)
    rows, full = depth // 2, wide + 2 * narrow
    vm = pl.BlockSpec(memory_space=pltpu.VMEM)
    fresh = [pltpu.with_memory_space_constraint(a, pltpu.VMEM) for a in (fresh_query, fresh_key, fresh_value)]
    early = pl.pallas_call(
        pack,
        out_shape=pltpu.VMEM((rows // 2, full), jnp.float32),
        in_specs=[vm] * 3,
        out_specs=vm,
        compiler_params=pltpu.CompilerParams(vmem_limit_bytes=8 << 20),
        name="pack",
    )(*fresh)
    early = lax.ppermute(early, "zero", both_ways())
    parts = [
        *(jnp.sum(a * a, axis=0, keepdims=True) for a in (fresh_query, fresh_key, fresh_value)),
        gain.astype(jnp.float32).reshape(1, -1),
    ]
    line = pl.pallas_call(
        join,
        out_shape=pltpu.VMEM((1, full + gain.size), jnp.float32),
        in_specs=[vm] * 4,
        out_specs=vm,
        compiler_params=pltpu.CompilerParams(vmem_limit_bytes=1 << 20),
        name="join",
    )(*(pltpu.with_memory_space_constraint(a, pltpu.VMEM) for a in parts))
    copies = jnp.broadcast_to(line, (CHIPS * CORES, line.size))
    everyone = lax.all_to_all(copies, "zero", split_axis=0, concat_axis=0, tiled=True)
    keep, give, late, *gives, q, k, v, q_out, k_out, v_out, gains = pl.pallas_call(
        normalise,
        out_shape=[pltpu.VMEM((rows, full), jnp.bfloat16)] * 2
        + [pltpu.VMEM((rows // 2, full), jnp.bfloat16)] * 3
        + [pltpu.VMEM((1, n), jnp.float32) for n in (wide, narrow, narrow)]
        + [jax.ShapeDtypeStruct((1, n), jnp.float32) for n in (wide, narrow, narrow)]
        + [pltpu.VMEM((2 * CHIPS * CORES, 2 * gain.size), jnp.bfloat16)],
        in_specs=[vm] * 4,
        out_specs=[vm] * 12,
        compiler_params=pltpu.CompilerParams(vmem_limit_bytes=8 << 20),
        name="normalise",
    )(everyone, *fresh)
    near = pl.pallas_call(
        receive,
        out_shape=pltpu.VMEM((rows // 2, full), jnp.bfloat16),
        in_specs=[vm] * 4,
        out_specs=vm,
        compiler_params=pltpu.CompilerParams(vmem_limit_bytes=8 << 20),
        name="receive",
    )(*(pltpu.with_memory_space_constraint(a, pltpu.VMEM) for a in (early, q, k, v)))

    size = CHIPS * CORES

    def swap(piece):
        return lax.ppermute(piece, "zero", other_core())

    have = {("a", 1): near, ("b", 0): late}
    have["c", 0], have["d", 0] = (swap(g) for g in gives)
    for kind in "abcd":
        for hop in range(1 + (kind == "a"), CHIPS):
            have[kind, hop] = lax.ppermute(have[kind, hop - 1], "zero", both_ways())
    hands = {"hand0": swap(keep)}
    for hop in range(1, CHIPS):
        for kind, pair in (("near", "ab"), ("far", "cd")):
            if hop == LAST and kind == "far":
                continue
            both = stacked(*(have[p, hop] for p in pair))
            hands[f"{kind}{hop}"] = swap(both)
    for kind in "cd":
        hands[f"{kind}{LAST}"] = swap(have[kind, LAST])

    def mine(kind, hop):
        return have[kind, hop], (hop, False, kind in "cd", "abcd".index(kind) % 2)

    def theirs(kind, hop):
        return hands[f"{kind}{hop}"], (hop, True, kind == "near", 0)

    puts = [
        [
            (keep, (0, False, False, 0)),
            (give, (0, True, False, 0)),
            (have["c", 0], (0, False, True, 0)),
            (have["d", 0], (0, False, True, 1)),
        ],
        [],
        [mine("a", 1), mine("a", 2), mine("b", 1), (hands["hand0"], (0, True, True, 0))],
        [],
        [],
    ]
    for hop in range(2, LAST):
        puts += [
            [],
            [mine(*p) for p in (("a", hop + 1), ("b", hop), ("c", hop - 1), ("d", hop - 1))]
            + [theirs(kind, hop - 1) for kind in ("near", "far")],
            [],
            [],
        ]
    puts += [
        [mine(*p) for p in (("b", LAST), ("c", LAST - 1), ("d", LAST - 1))]
        + [theirs(kind, LAST - 1) for kind in ("near", "far")],
        [theirs("near", LAST), mine("c", LAST)],
        [(hands[f"c{LAST}"], (LAST, True, False, 0)), mine("d", LAST)],
        [(hands[f"d{LAST}"], (LAST, True, False, 1))],
    ]

    shapes = [jax.ShapeDtypeStruct((depth * size, n), jnp.bfloat16) for n in (wide, narrow, narrow)]
    outs = None
    for some in puts:
        outs = placed([p for p, _ in some], [s for _, s in some], outs, shapes) if some else ticked(outs)
    serve_query, serve_key, serve_value = outs

    tp = lax.axis_size("tp")
    serve_norm = gains
    for k in (1, 2):
        theirs = lax.ppermute(serve_norm, "tp", [(i, i ^ k) for i in range(tp)])
        serve_norm += theirs
    serve_norm = serve_norm.reshape(-1)
    return (
        serve_query,
        serve_key,
        serve_value,
        *(column.reshape(-1) for column in (q_out, k_out, v_out)),
        serve_norm,
        fresh_query,
        fresh_key,
        fresh_value,
    )


def solution(mesh):
    in_specs = (
        P(("job", "zero"), "tp"),
        P(("job", "zero"), "tp"),
        P(("job", "zero"), "tp"),
        P(("job", "zero"), "tp"),
        P(("job", "zero"), "tp"),
        P(("job", "zero"), "tp"),
        P(("job", "zero", "tp")),
        P(("job", "zero", "tp")),
    )
    out_specs = (
        P("job", "tp"),
        P("job", "tp"),
        P("job", "tp"),
        P(("job", "tp")),
        P(("job", "tp")),
        P(("job", "tp")),
        P("job"),
        P(("job", "zero"), "tp"),
        P(("job", "zero"), "tp"),
        P(("job", "zero"), "tp"),
    )
    return jax.shard_map(body, mesh=mesh, in_specs=in_specs, out_specs=out_specs, check_vma=False)
```
